32 devices in a mesh: row: 4 (over z), col: 8 (over y, x, core).
Axes of the slice: x: 2, y: 2, z: 4, core: 2. Of those that a mesh axis runs over, the one named last changes fastest.
Arguments:
- matrix: float32 [32, 512, 16, 1024], P(None, 'row', None, 'col'), may hold values from -150 to 150
- inverse_rest: float32 [32, 512, 14, 1024], P(None, 'row', None, 'col'), may hold values from -6 to 6
- upper_block: float32 [4, 512, 2, 1024], P(None, 'row', None, 'col'), may hold values from -6 to 6, as said below
- lower_below: float32 [4, 512, 14, 1024], P(None, 'row', None, 'col'), may hold values from -0.046875 to 0.046875
- lower_inverse: float32 [4, 512, 2048], P(None, 'row', 'col'), may hold values from -1 to 1, as said below
Outputs:
- plus_rows: float32 [4, 512, 16, 1024], P(None, 'row', None, 'col')
The draws below stay inside these ranges and needn't reach their ends.
Inputs may be any that keep to these rules, and one draw needn't show every extreme that they name: `upper_block`: upper triangular. `lower_inverse`: unit lower triangular.
All inputs are finite; a program needn't handle non-finite values.
Results may differ from the reference program's by a relative error of at most 0.000052.
Values sent between devices are 32-bit elements; how exact they have to be, the bound alone decides.
No kernel may reach another device: no remote copies, remote signals or barrier semaphores. Data moves between devices by JAX's collectives and lax.ppermute only.
A program may use at most 256 MiB of HBM per device.

```python
import jax
import jax.numpy as jnp
from jax import lax

N = 16384
BLK = 128
W = 2048
REST = 14336
KR = 32
KC = 16
KWR = 4
KW = 2
KCR = 14
N_ROW = 4
N_COL = 8


def draw_matrix(key, part):
    row_key, col_key, base_key = jax.random.split(jax.random.fold_in(key, 17), 3)
    row_scale = jnp.exp(jax.random.uniform(row_key, (N, 1), jnp.float32, 0.0, 2.302585))
    col_scale = jnp.exp(jax.random.uniform(col_key, (1, N), jnp.float32, 0.0, 2.302585))
    values = jnp.clip(jax.random.normal(base_key, (N, N), jnp.float32), -6.0, 6.0)
    return (values * row_scale * col_scale * 0.25).reshape(KR, N // KR, KC, N // KC)


def draw_upper_block(key, part):
    base_key = jax.random.fold_in(key, 23)
    values = jnp.clip(jax.random.normal(base_key, (W, W), jnp.float32), -6.0, 6.0)
    return jnp.triu(values).reshape(KWR, W // KWR, KW, W // KW)


def draw_lower_inverse(key, part):
    base_key = jax.random.fold_in(key, 29)
    values = jnp.clip(jax.random.normal(base_key, (W, W), jnp.float32), -6.0, 6.0) * (0.5 / jnp.sqrt(W * 1.0))
    unit_lower = jnp.eye(W, dtype=jnp.float32) + jnp.tril(values, -1)
    return unit_lower.reshape(KWR, W // KWR, W)


def block_levels(own_key, extent, cuts, smallest, largest):
    loudness = 1.0
    for axis_at, blocks in cuts:
        draws = jax.random.uniform(jax.random.fold_in(jax.random.fold_in(own_key, 6), axis_at), (blocks,), jnp.float32, smallest / len(cuts), largest / len(cuts))
        loudness = loudness * jnp.repeat(jnp.exp(draws), extent[axis_at] // blocks).reshape((-1,) + (1,) * (len(extent) - 1 - axis_at))
    return loudness


def noise(key, dims, spread, reach, pieces=(), held_as=jnp.bfloat16):
    values = spread * jax.random.normal(key, dims, jnp.float32)
    if pieces:
        values = values * block_levels(key, dims, pieces, -0.22, 0.18)
    return jnp.clip(values, -reach, reach).astype(held_as)


def setup_inputs(seed: int = 0) -> dict:
    seeds = jax.random.split(jax.random.key(seed), 6)
    matrix = draw_matrix(jax.random.fold_in(seeds[5], 71), 0)
    inverse_rest = noise(seeds[1], (KR, N_ROW * BLK, KCR, N_COL * BLK), 1.0, 6.0, ((1, 4), (3, 8)), jnp.float32)
    upper_block = draw_upper_block(jax.random.fold_in(seeds[5], 71), 0)
    lower_below = noise(seeds[3], (KWR, N_ROW * BLK, KCR, N_COL * BLK), REST ** -0.5, 0.046875, ((1, 4), (3, 8)), jnp.float32)
    lower_inverse = draw_lower_inverse(jax.random.fold_in(seeds[5], 71), 0)
    return {"matrix": matrix, "inverse_rest": inverse_rest, "upper_block": upper_block, "lower_below": lower_below, "lower_inverse": lower_inverse}


def reference(matrix, inverse_rest, upper_block, lower_below, lower_inverse):
    whole_matrix = matrix.reshape(N, N)
    rest_inverse = inverse_rest.reshape(N, N - W)
    upper_part = upper_block.reshape(W, W)
    below_part = lower_below.reshape(W, N - W)
    factor_part = lower_inverse.reshape(W, W)
    correction = jnp.dot(rest_inverse, below_part.T, precision=lax.Precision.HIGHEST, preferred_element_type=jnp.float32)
    update_panel = jnp.concatenate([upper_part, jnp.zeros((N - W, W), jnp.float32)], axis=0) - correction
    inverse_panel = jnp.dot(update_panel, factor_part, precision=lax.Precision.HIGHEST, preferred_element_type=jnp.float32)
    matrix_norm = jnp.sum(whole_matrix * whole_matrix)
    inverse_norm = jnp.sum(rest_inverse * rest_inverse) + jnp.sum(inverse_panel * inverse_panel)
    balance = jnp.sqrt(jnp.sqrt(inverse_norm / matrix_norm))
    plus_rows = 0.5 * (balance * whole_matrix[:W] + inverse_panel.T / balance)
    return plus_rows.reshape(KWR, W // KWR, KC, N // KC)
```

```python
import functools

import jax
import jax.numpy as jnp
from jax import lax
from jax.experimental import pallas as pl
from jax.experimental.pallas import tpu as pltpu
from jax.sharding import PartitionSpec as P


PARTS = 2
AHEAD = 4
LIMIT = 48 * 1024 * 1024


def dot_split(left, right, form):
    return jnp.einsum(
        form, left, right, precision=lax.Precision.HIGH, preferred_element_type=jnp.float32
    )


def after(value, token):
    return lax.optimization_barrier((value, token))[0]


def halves(value):
    high = value.astype(jnp.bfloat16)
    return high, (value - high.astype(jnp.float32)).astype(jnp.bfloat16)


def split_kernel(which_ref, rest_ref, out_ref, sum_ref):
    cycles, blk = rest_ref.shape[1], rest_ref.shape[3]
    depth = cycles * blk
    squares = jnp.zeros((8, blk), jnp.float32)
    for m in range(cycles):
        value = rest_ref[0, m]
        high, low = halves(value)
        out_ref[:, m * blk : (m + 1) * blk] = high
        out_ref[:, depth + m * blk : depth + (m + 1) * blk] = low
        squares = squares + jnp.sum((value * value).reshape(-1, 8, blk), axis=0)
    sum_ref[0] = squares


def split_rows(rest, which, group, ratio, half_rows):
    blk, cycles = rest.shape[2], rest.shape[1]
    depth = cycles * blk
    chips = ratio * half_rows
    count = chips * group

    def source(i, which_ref):
        u, qh, g = i // (half_rows * group), (i // group) % half_rows, i % group
        return (((qh * 2 + which_ref[0]) * group + g) * ratio + u, 0, 0, 0)

    return pl.pallas_call(
        split_kernel,
        grid_spec=pltpu.PrefetchScalarGridSpec(
            num_scalar_prefetch=1,
            grid=(count,),
            in_specs=[pl.BlockSpec((1, cycles, blk, blk), source)],
            out_specs=[
                pl.BlockSpec((blk, 2 * depth), lambda i, s: (i, 0)),
                pl.BlockSpec((1, 8, blk), lambda i, s: (i, 0, 0)),
            ],
        ),
        out_shape=[
            jax.ShapeDtypeStruct((count * blk, 2 * depth), jnp.bfloat16),
            jax.ShapeDtypeStruct((count, 8, blk), jnp.float32),
        ],
        compiler_params=pltpu.CompilerParams(vmem_limit_bytes=LIMIT),
        cost_estimate=pl.CostEstimate(
            flops=8 * count * blk * depth,
            bytes_accessed=8 * count * blk * depth,
            transcendentals=0,
        ),
    )(which, rest)


def product_kernel(rows, half_rows, order_ref, left_ref, upper_ref, *refs):
    blocks, (out_ref, high_ref, low_ref) = refs[:-3], refs[-3:]
    depth = high_ref.shape[1]
    blk = blocks[0].shape[1]
    parts = len(blocks) // rows
    row = order_ref[0]

    @pl.when(pl.program_id(0) == 0)
    def _():
        for step in range(rows):
            owner = lax.rem(row + rows - step, rows)
            at = pl.ds(pl.multiple_of(owner * blk, blk), blk)
            column = 0
            for p in range(parts):
                planes = blocks[step * parts + p]
                for m in range(planes.shape[0]):
                    high, low = halves(planes[m])
                    high_ref[at, column : column + blk] = high
                    low_ref[at, column : column + blk] = low
                    column += blk

    def dot(a, b):
        return lax.dot_general(
            a, b, (((1,), (1,)), ((), ())), preferred_element_type=jnp.float32
        )

    left_high, left_low = left_ref[:, :depth], left_ref[:, depth:]
    total = dot(left_high, high_ref[...])
    total += dot(left_low, high_ref[...])
    total += dot(left_high, low_ref[...])
    out_ref[0] = total

    first = lax.rem(order_ref[pl.program_id(0) + 3], half_rows) == 0

    @pl.when(jnp.logical_and(first, order_ref[2] == 1))
    def _():
        column = pl.ds(pl.multiple_of(order_ref[1] * blk, blk), blk)
        for g in range(upper_ref.shape[2]):
            at = slice(g * blk, (g + 1) * blk)
            out_ref[0, at, column] = out_ref[0, at, column] - upper_ref[0, 0, g]


def product(left, upper, layer, blocks, order, rows, chips):
    depth = left.shape[1] // 2
    span = blocks[0].shape[1] * rows
    share = left.shape[0] // chips
    whole = [pl.BlockSpec(b.shape, lambda k, s: (0, 0, 0)) for b in blocks]
    return pl.pallas_call(
        functools.partial(product_kernel, rows, rows // 2),
        grid_spec=pltpu.PrefetchScalarGridSpec(
            num_scalar_prefetch=1,
            grid=(chips,),
            in_specs=[
                pl.BlockSpec((share, 2 * depth), lambda k, s: (s[k + 3], 0)),
                pl.BlockSpec(
                    (1, 1) + upper.shape[2:],
                    lambda k, s: (layer, s[k + 3] // (rows // 2), 0, 0, 0),
                ),
            ]
            + whole,
            out_specs=pl.BlockSpec((1, share, span), lambda k, s: (k, 0, 0)),
            scratch_shapes=[
                pltpu.VMEM((span, depth), jnp.bfloat16),
                pltpu.VMEM((span, depth), jnp.bfloat16),
            ],
        ),
        out_shape=jax.ShapeDtypeStruct((chips, share, span), jnp.float32),
        compiler_params=pltpu.CompilerParams(vmem_limit_bytes=LIMIT),
        cost_estimate=pl.CostEstimate(
            flops=6 * chips * share * span * depth,
            bytes_accessed=4 * chips * share * (depth + span),
            transcendentals=0,
        ),
    )(order, left, upper, *blocks)


def partner(chip, k, chips):
    return chip ^ k if chips & (chips - 1) == 0 else (chip + k) % chips


def total_over(value, axis, count):
    if count & (count - 1):
        return lax.psum(value, axis)
    bit = 1
    while bit < count:
        value = value + lax.ppermute(value, axis, [(i, i ^ bit) for i in range(count)])
        bit *= 2
    return value


def per_device(matrix, inverse_rest, upper_block, lower_below, lower_inverse):
    rows = lax.axis_size("row")
    cols = lax.axis_size("col")
    row = lax.axis_index("row")
    col = lax.axis_index("col")
    ratio = cols // rows
    blk = matrix.shape[1]
    col_cycles = matrix.shape[2]
    panel_cycles = lower_inverse.shape[0]
    group = col_cycles // rows
    chips = cols // 2
    half_rows = rows // 2
    high, place = col // rows, col % rows
    core, chip = col % 2, col // 2
    share = group * blk
    span = rows * blk
    planes = inverse_rest.shape[2]
    cuts = [planes * p // PARTS for p in range(PARTS + 1)]
    cycles = list(reversed(range(panel_cycles)))

    ring = [(i, (i + 1) % rows) for i in range(rows)]
    flat = lower_below.transpose(0, 2, 1, 3)
    rest = inverse_rest.transpose(0, 2, 1, 3)
    sent = []
    panels = {}
    for cycle in cycles:
        held = [flat[cycle, cuts[p] : cuts[p + 1]] for p in range(PARTS)]
        panels[cycle] = list(held)
        for step in range(1, rows):
            for p in range(PARTS):
                block = held[p]
                if step == 1 and len(sent) >= AHEAD:
                    block = after(block, sent[-AHEAD])
                held[p] = lax.ppermute(block, "row", ring)
                sent.append(held[p])
                panels[cycle].append(held[p])

    factor_rows = lax.all_gather(lower_inverse, "row", axis=1, tiled=True)
    factor = lax.all_gather(factor_rows, "col", axis=0)

    left_send, squares_send = split_rows(rest, (1 - core)[None], group, ratio, half_rows)
    left_keep, squares_keep = split_rows(rest, core[None], group, ratio, half_rows)
    upper_cycles = panel_cycles // ratio
    upper = upper_block.reshape(upper_cycles, ratio, blk, -1, blk).transpose(3, 1, 0, 2, 4)
    matrix_sq = jnp.sum(matrix * matrix)
    row_early = after(row, matrix_sq)

    def order(cycle, active):
        active = jnp.logical_and(active, high == cycle % ratio).astype(jnp.int32)
        return jnp.stack(
            [row_early, place, active] + [partner(chip, k, chips) for k in range(chips)]
        )


    swap = [(i, i ^ 1) for i in range(cols)]
    gone, kept, shared = {}, {}, {}
    for cycle in cycles:
        layer = cycle // ratio
        gone = product(left_send, upper, layer, panels[cycle], order(cycle, core == 1), rows, chips)
        there = lax.ppermute(gone, "col", swap)
        kept[cycle] = product(
            left_keep, upper, layer, panels[cycle], order(cycle, core == 0), rows, chips,
        )
        shared[cycle] = [kept[cycle][0] + there[0]]
        for k in range(1, chips):
            shared[cycle].append(
                lax.ppermute(
                    kept[cycle][k] + there[k],
                    "col",
                    [(i, partner(i // 2, k, chips) * 2 + i % 2) for i in range(cols)],
                )
            )

    def mirror(out):
        arrived = []
        for k in range(rows):
            pairs = []
            for r in range(rows):
                for c in range(cols):
                    pairs.append(
                        (r * cols + c, ((c % rows + k) % rows) * cols + (c // rows) * rows + r)
                    )
            block = lax.dynamic_index_in_dim(out, (place + k) % rows, 1, keepdims=False)
            arrived.append(lax.ppermute(block, ("row", "col"), pairs))
        stacked = jnp.stack(arrived)
        ordered = [
            lax.dynamic_index_in_dim(stacked, (row - q) % rows, 0, keepdims=False)
            for q in range(rows)
        ]
        return jnp.stack(ordered, axis=2).reshape(-1, blk, col_cycles, blk)

    updates = {}
    totals = []
    results = []
    waiting = []
    width = span // factor.shape[3]
    for cycle in cycles:
        parts = shared[cycle]
        if cycle:
            parts = after(parts, kept[cycle - 1])
        total = sum(parts[1:], parts[0])
        if cycle == 0:
            total = after(total, results)
        updates[cycle] = total

        wide = factor[cycle * width : (cycle + 1) * width]
        out = jnp.zeros((), jnp.float32)
        for later in reversed(range(cycle, panel_cycles)):
            out = out + dot_split(wide[:, later], updates[later], "ctw,it->cwi")
        totals.append(jnp.sum(out * out))
        out = out.reshape(1, rows, blk, share)
        if cycle == 0:
            rest_sq = jnp.sum(squares_send) + jnp.sum(squares_keep)
            sums = jnp.stack([matrix_sq, rest_sq + sum(totals)])
            sums = jnp.broadcast_to(sums[:, None, None], (2, 8, blk))
            sums = total_over(sums, "row", rows)
            out = after(out, sums)
            sums = total_over(sums, "col", cols)
        waiting.insert(0, out)
        if cycle <= 2:
            results.insert(0, mirror(jnp.concatenate(waiting, axis=0)))
            waiting = []

    balance = jnp.sqrt(jnp.sqrt(sums[1, 0, 0] / sums[0, 0, 0]))
    mirrored = jnp.concatenate(results, axis=0)
    return 0.5 * (balance * matrix[:panel_cycles] - mirrored / balance)


def solution(mesh):
    in_specs = (
        P(None, "row", None, "col"),
        P(None, "row", None, "col"),
        P(None, "row", None, "col"),
        P(None, "row", None, "col"),
        P(None, "row", "col"),
    )
    out_specs = P(None, "row", None, "col")

    def whole(matrix, inverse_rest, upper_block, lower_below, lower_inverse):
        return jax.shard_map(
            per_device, mesh=mesh, in_specs=in_specs, out_specs=out_specs, check_vma=False
        )(matrix, inverse_rest, upper_block, lower_below, lower_inverse)

    return whole
```

```python
import functools

import jax
import jax.numpy as jnp
from jax import lax
from jax.experimental import pallas as pl
from jax.experimental.pallas import tpu as pltpu
from jax.sharding import PartitionSpec as P


PARTS = 2
HALVED = 1
AHEAD = 4
LIMIT = 48 * 1024 * 1024


def after(value, token):
    return lax.optimization_barrier((value, token))[0]


def halves(value):
    high = value.astype(jnp.bfloat16)
    return high, (value - high.astype(jnp.float32)).astype(jnp.bfloat16)


def split_kernel(which_ref, rest_ref, out_ref, sum_ref):
    cycles, blk = rest_ref.shape[1], rest_ref.shape[3]
    depth = cycles * blk
    squares = jnp.zeros((8, blk), jnp.float32)
    for m in range(cycles):
        value = rest_ref[0, m]
        high, low = halves(value)
        out_ref[:, m * blk : (m + 1) * blk] = high
        out_ref[:, depth + m * blk : depth + (m + 1) * blk] = low
        squares = squares + jnp.sum((value * value).reshape(-1, 8, blk), axis=0)
    sum_ref[0] = squares


def split_rows(rest, which, group, ratio, half_rows):
    blk, cycles = rest.shape[2], rest.shape[1]
    depth = cycles * blk
    chips = ratio * half_rows
    count = chips * group

    def source(i, which_ref):
        u, qh, g = i // (half_rows * group), (i // group) % half_rows, i % group
        return (((qh * 2 + which_ref[0]) * group + g) * ratio + u, 0, 0, 0)

    return pl.pallas_call(
        split_kernel,
        grid_spec=pltpu.PrefetchScalarGridSpec(
            num_scalar_prefetch=1,
            grid=(count,),
            in_specs=[pl.BlockSpec((1, cycles, blk, blk), source)],
            out_specs=[
                pl.BlockSpec((blk, 2 * depth), lambda i, s: (i, 0)),
                pl.BlockSpec((1, 8, blk), lambda i, s: (i, 0, 0)),
            ],
        ),
        out_shape=[
            jax.ShapeDtypeStruct((count * blk, 2 * depth), jnp.bfloat16),
            jax.ShapeDtypeStruct((count, 8, blk), jnp.float32),
        ],
        compiler_params=pltpu.CompilerParams(vmem_limit_bytes=LIMIT),
        cost_estimate=pl.CostEstimate(
            flops=8 * count * blk * depth,
            bytes_accessed=8 * count * blk * depth,
            transcendentals=0,
        ),
    )(which, rest)


def product_kernel(rows, half_rows, whole, order_ref, left_ref, upper_ref, *refs):
    blocks, (out_ref, high_ref, low_ref) = refs[:-3], refs[-3:]
    depth = high_ref.shape[1]
    blk = blocks[0].shape[1]
    count = len(blocks) // PARTS
    row = order_ref[0]

    @pl.when(pl.program_id(0) == 0)
    def _():
        for step in range(count):
            owner = lax.rem(row + rows - step, rows) if whole else step
            at = pl.ds(pl.multiple_of(owner * blk, blk), blk)
            column = 0
            for p in range(PARTS):
                planes = blocks[step * PARTS + p]
                for m in range(planes.shape[0]):
                    high, low = halves(planes[m])
                    high_ref[at, column : column + blk] = high
                    low_ref[at, column : column + blk] = low
                    column += blk

    def dot(a, b):
        return lax.dot_general(
            a, b, (((1,), (1,)), ((), ())), preferred_element_type=jnp.float32
        )

    left_high, left_low = left_ref[:, :depth], left_ref[:, depth:]
    total = dot(left_high, high_ref[...])
    total += dot(left_low, high_ref[...])
    total += dot(left_high, low_ref[...])
    out_ref[0] = total

    first = lax.rem(order_ref[pl.program_id(0) + 3], half_rows) == 0

    @pl.when(jnp.logical_and(first, order_ref[2] == 1))
    def _():
        column = pl.ds(pl.multiple_of(order_ref[1] * blk, blk), blk)
        for g in range(upper_ref.shape[2]):
            at = slice(g * blk, (g + 1) * blk)
            out_ref[0, at, column] = out_ref[0, at, column] - upper_ref[0, 0, g]


def product(left, upper, layer, blocks, order, rows, chips):
    depth = left.shape[1] // 2
    count = len(blocks) // PARTS
    span = blocks[0].shape[1] * count
    share = left.shape[0] // chips
    whole = [pl.BlockSpec(b.shape, lambda k, s: (0, 0, 0)) for b in blocks]
    return pl.pallas_call(
        functools.partial(product_kernel, rows, rows // 2, count == rows),
        grid_spec=pltpu.PrefetchScalarGridSpec(
            num_scalar_prefetch=1,
            grid=(chips,),
            in_specs=[
                pl.BlockSpec((share, 2 * depth), lambda k, s: (s[k + 3], 0)),
                pl.BlockSpec(
                    (1, 1) + upper.shape[2:],
                    lambda k, s: (layer, s[k + 3] // (rows // 2), 0, 0, 0),
                ),
            ]
            + whole,
            out_specs=pl.BlockSpec((1, share, span), lambda k, s: (k, 0, 0)),
            scratch_shapes=[
                pltpu.VMEM((span, depth), jnp.bfloat16),
                pltpu.VMEM((span, depth), jnp.bfloat16),
            ],
        ),
        out_shape=jax.ShapeDtypeStruct((chips, share, span), jnp.float32),
        compiler_params=pltpu.CompilerParams(vmem_limit_bytes=LIMIT),
        cost_estimate=pl.CostEstimate(
            flops=6 * chips * share * span * depth,
            bytes_accessed=4 * chips * share * (depth + span),
            transcendentals=0,
        ),
    )(order, left, upper, *blocks)


def panel_kernel(rows, count, groups, parts, row_ref, *refs):
    shares, refs = refs[: groups * parts], refs[groups * parts :]
    factors, refs = refs[:count], refs[count:]
    older, refs = refs[: 2 * (count - 1)], refs[2 * (count - 1) :]
    high_ref, low_ref, out_ref, sum_ref, factor_high, factor_low = refs
    width, wide = factors[0].shape[0], factors[0].shape[3]

    @pl.when(pl.program_id(0) == 0)
    def _():
        sum_ref[...] = jnp.zeros_like(sum_ref)
        for n in range(count):
            for j in range(width):
                columns = slice(j * wide, (j + 1) * wide)
                if n or groups == 1:
                    high, low = halves(factors[n][j, 0])
                    factor_high[n, :, columns] = high
                    factor_low[n, :, columns] = low
                    continue
                blk = factors[n].shape[2] // rows
                for step in range(rows):
                    owner = lax.rem(row_ref[0] + rows - step, rows)
                    at = pl.ds(pl.multiple_of(owner * blk, blk), blk)
                    high, low = halves(factors[n][j, 0, at, :])
                    factor_high[n, step * blk : (step + 1) * blk, columns] = high
                    factor_low[n, step * blk : (step + 1) * blk, columns] = low

    def dot(a, b):
        return jnp.dot(a, b, preferred_element_type=jnp.float32)

    sums = []
    for g in range(groups):
        total = shares[g * parts][...]
        for p in range(1, parts):
            total = total + shares[g * parts + p][...]
        sums.append(total)
    total = jnp.concatenate(sums, axis=1) if groups > 1 else sums[0]
    high, low = halves(total)
    high_ref[...] = high
    low_ref[...] = low
    pairs = [(high, low)] + [
        (older[2 * n][...], older[2 * n + 1][...]) for n in range(count - 1)
    ]
    panel = jnp.zeros((total.shape[0], factor_high.shape[2]), jnp.float32)
    for n, (high, low) in enumerate(pairs):
        panel += dot(high, factor_high[n])
        panel += dot(low, factor_high[n])
        panel += dot(high, factor_low[n])
    sum_ref[...] += jnp.sum((panel * panel).reshape(-1, 8, panel.shape[1]), axis=0)
    out_ref[...] = panel.T.reshape(out_ref.shape)


def panel_columns(shares, factor, row, cycle, later, older, rows):
    groups, parts = len(shares), len(shares[0])
    shares = [x for group in shares for x in group]
    own, piece = shares[0].shape
    span = piece * groups
    blk = span // rows
    width = span // factor.shape[3]
    count = len(later)
    step = min(own, 128)
    slab = pl.BlockSpec((step, span), lambda i, s: (i, 0))
    part = pl.BlockSpec((step, piece), lambda i, s: (i, 0))
    pieces = [
        pl.BlockSpec(
            (width, 1, span, factor.shape[3]), functools.partial(lambda n, i, s: (cycle, n, 0, 0), n)
        )
        for n in later
    ]
    flat = [x for pair in older for x in pair]
    return pl.pallas_call(
        functools.partial(panel_kernel, rows, count, groups, parts),
        grid_spec=pltpu.PrefetchScalarGridSpec(
            num_scalar_prefetch=1,
            grid=(own // step,),
            in_specs=[part] * len(shares) + pieces + [slab] * len(flat),
            out_specs=[
                slab,
                slab,
                pl.BlockSpec((1, rows, blk, step), lambda i, s: (0, 0, 0, i)),
                pl.BlockSpec((8, span), lambda i, s: (0, 0)),
            ],
            scratch_shapes=[
                pltpu.VMEM((count, span, span), jnp.bfloat16),
                pltpu.VMEM((count, span, span), jnp.bfloat16),
            ],
        ),
        out_shape=[
            jax.ShapeDtypeStruct((own, span), jnp.bfloat16),
            jax.ShapeDtypeStruct((own, span), jnp.bfloat16),
            jax.ShapeDtypeStruct((1, rows, blk, own), jnp.float32),
            jax.ShapeDtypeStruct((8, span), jnp.float32),
        ],
        compiler_params=pltpu.CompilerParams(vmem_limit_bytes=LIMIT),
        cost_estimate=pl.CostEstimate(
            flops=6 * count * own * span * span,
            bytes_accessed=4 * own * span * (len(shares) + count + 2),
            transcendentals=0,
        ),
    )(row[None], *shares, *([factor] * count), *flat)


def partner(chip, k, chips):
    return chip ^ k if chips & (chips - 1) == 0 else (chip + k) % chips


def total_over(value, axis, count):
    if count & (count - 1):
        return lax.psum(value, axis)
    bit = 1
    while bit < count:
        value = value + lax.ppermute(value, axis, [(i, i ^ bit) for i in range(count)])
        bit *= 2
    return value


def per_device(matrix, inverse_rest, upper_block, lower_below, lower_inverse):
    rows = lax.axis_size("row")
    cols = lax.axis_size("col")
    row = lax.axis_index("row")
    col = lax.axis_index("col")
    ratio = cols // rows
    blk = matrix.shape[1]
    col_cycles = matrix.shape[2]
    panel_cycles = lower_inverse.shape[0]
    group = col_cycles // rows
    chips = cols // 2
    half_rows = rows // 2
    high, place = col // rows, col % rows
    core, chip = col % 2, col // 2
    planes = inverse_rest.shape[2]
    cuts = [planes * p // PARTS for p in range(PARTS + 1)]
    cycles = list(reversed(range(panel_cycles)))

    ring = [(i, (i + 1) % rows) for i in range(rows)]
    flat = lower_below.transpose(0, 2, 1, 3)
    rest = inverse_rest.transpose(0, 2, 1, 3)
    sent = []
    panels = {}
    for cycle in cycles:
        held = [flat[cycle, cuts[p] : cuts[p + 1]] for p in range(PARTS)]
        panels[cycle] = list(held)
        for step in range(1, rows):
            for p in range(PARTS):
                block = held[p]
                if step == 1 and len(sent) >= AHEAD:
                    block = after(block, sent[-AHEAD])
                held[p] = lax.ppermute(block, "row", ring)
                sent.append(held[p])
                panels[cycle].append(held[p])

    factor_rows = lax.all_gather(lower_inverse, "row", axis=1, tiled=True)
    factor = lax.all_gather(factor_rows, "col", axis=0)

    left_send, squares_send = split_rows(rest, (1 - core)[None], group, ratio, half_rows)
    left_keep, squares_keep = split_rows(rest, core[None], group, ratio, half_rows)
    upper_cycles = panel_cycles // ratio
    upper = upper_block.reshape(upper_cycles, ratio, blk, -1, blk).transpose(3, 1, 0, 2, 4)
    matrix_sq = jnp.sum(matrix * matrix)
    row_early = after(row, matrix_sq)

    def order(chunk, active):
        cycle, first, count = chunk
        at = place if count == rows else (row - place) % rows - first
        active = jnp.logical_and(active, high == cycle % ratio)
        active = jnp.logical_and(active, jnp.logical_and(at >= 0, at < count))
        return jnp.stack(
            [row_early, jnp.clip(at, 0, count - 1), active.astype(jnp.int32)]
            + [partner(chip, k, chips) for k in range(chips)]
        )

    swap = [(i, i ^ 1) for i in range(cols)]
    kept, shared = {}, {}
    chunks = chunks_of(rows, panel_cycles)
    for chunk in chunks:
        cycle, first, count = chunk
        layer = cycle // ratio
        blocks = panels[cycle][first * PARTS : (first + count) * PARTS]
        gone = product(left_send, upper, layer, blocks, order(chunk, core == 1), rows, chips)
        there = lax.ppermute(gone, "col", swap)
        mine = product(left_keep, upper, layer, blocks, order(chunk, core == 0), rows, chips)
        kept[cycle] = mine
        added = [mine[k] + there[k] for k in range(chips)]
        shared[chunk] = [added[0]]
        for k in range(1, chips):
            shared[chunk].append(
                lax.ppermute(
                    added[k],
                    "col",
                    [(i, partner(i // 2, k, chips) * 2 + i % 2) for i in range(cols)],
                )
            )

    def mirror(out):
        arrived = []
        for k in range(rows):
            pairs = []
            for r in range(rows):
                for c in range(cols):
                    pairs.append(
                        (r * cols + c, ((c % rows + k) % rows) * cols + (c // rows) * rows + r)
                    )
            block = lax.dynamic_index_in_dim(out, (place + k) % rows, 1, keepdims=False)
            arrived.append(lax.ppermute(block, ("row", "col"), pairs))
        stacked = jnp.stack(arrived)
        ordered = [
            lax.dynamic_index_in_dim(stacked, (row - q) % rows, 0, keepdims=False)
            for q in range(rows)
        ]
        return jnp.stack(ordered, axis=2).reshape(-1, blk, col_cycles, blk)

    updates = {}
    totals = []
    results = []
    waiting = []
    for cycle in cycles:
        parts = [shared[chunk] for chunk in chunks if chunk[0] == cycle]
        if cycle:
            parts = after(parts, kept[cycle - 1])
        if cycle == 0:
            parts = after(parts, results)

        later = [cycle] + list(updates)
        high_part, low_part, out, square = panel_columns(
            parts, factor, row, cycle, later, list(updates.values()), rows
        )
        updates[cycle] = (high_part, low_part)
        totals.append(jnp.sum(square))
        if cycle == 0:
            rest_sq = jnp.sum(squares_send) + jnp.sum(squares_keep)
            sums = jnp.stack([matrix_sq, rest_sq + sum(totals)])
            sums = jnp.broadcast_to(sums[:, None, None], (2, 8, blk))
            sums = total_over(sums, "row", rows)
            out = after(out, sums)
            sums = total_over(sums, "col", cols)
        waiting.insert(0, out)
        if cycle <= 2:
            results.insert(0, mirror(jnp.concatenate(waiting, axis=0)))
            waiting = []

    balance = jnp.sqrt(jnp.sqrt(sums[1, 0, 0] / sums[0, 0, 0]))
    mirrored = jnp.concatenate(results, axis=0)
    return 0.5 * (balance * matrix[:panel_cycles] - mirrored / balance)


def chunks_of(rows, panel_cycles):
    half = rows // 2
    chunks = []
    for cycle in reversed(range(panel_cycles)):
        if cycle < HALVED:
            chunks += [(cycle, 0, half), (cycle, half, half)]
        else:
            chunks += [(cycle, 0, rows)]
    return chunks


def solution(mesh):
    in_specs = (
        P(None, "row", None, "col"),
        P(None, "row", None, "col"),
        P(None, "row", None, "col"),
        P(None, "row", None, "col"),
        P(None, "row", "col"),
    )
    out_specs = P(None, "row", None, "col")

    def whole(matrix, inverse_rest, upper_block, lower_below, lower_inverse):
        return jax.shard_map(
            per_device, mesh=mesh, in_specs=in_specs, out_specs=out_specs, check_vma=False
        )(matrix, inverse_rest, upper_block, lower_below, lower_inverse)

    return whole
```
